32 devices in a mesh: lat: 4 (over y, core), lon: 8 (over z, x).
Axes of the slice: x: 2, y: 2, z: 4, core: 2. Of those that a mesh axis runs over, the one named last changes fastest.
Arguments:
- layer_temp: float32 [64, 35, 1024], P('lat', None, 'lon'), may hold values from -20 to -2
- ice_depth_per_class: float32 [64, 5, 1024], P('lat', None, 'lon'), may hold values from 0.5 to 3
- ice_area: float32 [64, 5, 1024], P('lat', None, 'lon'), may hold values from 0.05 to 0.2
- surf_temp: float32 [64, 1024], P('lat', 'lon'), may hold values from -30 to -2
- seawater_thermal_input: float32 [64, 1024], P('lat', 'lon'), may hold values from 0 to 0.3
- velocity: float32 [2, 64, 1024], P(None, 'lat', 'lon'), may hold values from -1.2 to 1.2
- stress: float32 [3, 64, 1024], P(None, 'lat', 'lon'), may hold values from -3 to 3
- wind_stress: float32 [2, 64, 1024], P(None, 'lat', 'lon'), may hold values from -1.8 to 1.8
- current: float32 [2, 64, 1024], P(None, 'lat', 'lon'), may hold values from -1.8 to 1.8
- land_mask: int32 [64, 1024], P('lat', 'lon'), may hold values 0 or 1
- ice_mask: int32 [8, 64], P('lon', 'lat'), may hold values from 0 to 1, as said below
- band_index: int32 [64], P('lat'), may hold values from 0 to 15, as said below
Outputs:
- temp_after: float32 [64, 35, 1024], P('lat', None, 'lon')
- thick_after: float32 [64, 5, 1024], P('lat', None, 'lon')
- velocity_after: float32 [2, 64, 1024], P(None, 'lat', 'lon')
- stress_after: float32 [3, 64, 1024], P(None, 'lat', 'lon')
- zonal_volume: float32 [16], P('lat')
The draws below stay inside these ranges and needn't reach their ends.
Inputs may be any that keep to these rules, and one draw needn't show every extreme that they name: `ice_mask`: for each lat index, the strips of all devices with that index include at most 56 ice-covered strips and more than (6) times the number of lon devices; among these devices one has all its 16 strips ice-covered. `band_index`: every band holds 1 to 7 rows, which lie next to one another; one band holds exactly 7.
All inputs are finite; a program needn't handle non-finite values. No bound on the sum of `land_mask` on one device may be relied on, other than what follows from the above.
Results may differ from the reference program's by a relative error of at most 0.00002.
Values sent between devices are 32-bit elements; how exact they have to be, the bound alone decides.
A program may use at most 64 MiB of HBM per device.

```python
import math
import jax
import jax.numpy as jnp
from jax import lax

DEPTH_CLASSES = 5
VERTICAL_LEVELS = 7
ROWS_DEV = 16
COLS_DEV = 128
SUBCYCLES = 3
SWEEPS = 2
ICE_DEV = 7
GRID_ROWS = 64
GRID_COLS = 1024
BANDS = 16
N_LAT = 4
N_LON = 8


def ice_row_group(group_key):
    count_key, full_key, shuffle_key = jax.random.split(group_key, 3)
    strip_total = N_LON * ROWS_DEV
    ice_total = N_LON * (ICE_DEV - 1) + jax.random.randint(count_key, (), 1, N_LON + 1)
    full_device = jax.random.randint(full_key, (), 0, N_LON)
    shuffled = jax.random.permutation(shuffle_key, strip_total)
    owner_lon = jnp.arange(strip_total, dtype=jnp.int32) // ROWS_DEV
    priority = jnp.where(owner_lon == full_device, shuffled - strip_total, shuffled)
    position = jnp.argsort(jnp.argsort(priority, stable=True), stable=True)
    return (position < ice_total).astype(jnp.int32).reshape(N_LON, ROWS_DEV)


def draw_ice_mask(key, part):
    row_keys = jax.random.split(jax.random.fold_in(key, 7), N_LAT)
    grouped = jax.vmap(ice_row_group)(row_keys)
    return jnp.transpose(grouped, (1, 0, 2)).reshape(N_LON, N_LAT * ROWS_DEV)


def draw_band_index(key, part):
    shift_key, pick_key, pair_key = jax.random.split(jax.random.fold_in(key, 11), 3)
    base_rows = ROWS_DEV // 4
    pair_count = BANDS // 2
    moved = jax.random.randint(shift_key, (pair_count,), -(base_rows - 1), base_rows)
    chosen_pair = jax.random.randint(pick_key, (), 0, pair_count)
    moved = jnp.where(jnp.arange(pair_count, dtype=jnp.int32) == chosen_pair, base_rows - 1, moved)
    shuffled = jax.random.permutation(pair_key, BANDS).astype(jnp.int32)
    place = jnp.argsort(shuffled, stable=True).astype(jnp.int32)
    pair_of_band = place // 2
    side = place % 2
    band_rows = (base_rows + moved[pair_of_band] * (1 - 2 * side)).astype(jnp.int32)
    band_ends = jnp.cumsum(band_rows)
    row_ids = jnp.arange(GRID_ROWS, dtype=jnp.int32)
    upward = jnp.sum((band_ends[None, :] <= row_ids[:, None]).astype(jnp.int32), axis=1)
    return ((upward + BANDS // 2) % BANDS).astype(jnp.int32)


def place_ends(entries, key, low, top_value):
    shape = entries.shape
    index_at = [jax.random.randint(jax.random.fold_in(key, axis), (), 0, shape[axis]) for axis in range(len(shape))]
    entries = entries.at[tuple(index_at)].set(low)
    longest = shape.index(max(shape))
    index_at[longest] = (index_at[longest] + 1) % shape[longest]
    return entries.at[tuple(index_at)].set(top_value)


def shard_levels(stream_key, dims, cuts, least, largest):
    def one(axis_at, parts):
        steps = jax.random.uniform(jax.random.fold_in(jax.random.fold_in(stream_key, 6), axis_at), (parts,), jnp.float32, least / len(cuts), largest / len(cuts))
        return jnp.repeat(jnp.exp(steps), dims[axis_at] // parts).reshape((-1,) + (1,) * (len(dims) - axis_at - 1))

    level = one(*cuts[0])
    for cut in cuts[1:]:
        level = level * one(*cut)
    return level


def gaussian(rng, shape, spread, reach, cuts=(), kind=jnp.bfloat16):
    result = spread * jax.random.normal(rng, shape, jnp.float32)
    if cuts:
        result = result * shard_levels(rng, shape, cuts, -0.22, 0.18)
    return jnp.clip(result, -reach, reach).astype(kind)


def setup_inputs(seed: int = 0) -> dict:
    streams_of = jax.random.split(jax.random.key(seed), 13)
    layer_temp = jnp.clip(-20.0 + 18.0 * jax.random.uniform(streams_of[0], (GRID_ROWS, DEPTH_CLASSES * VERTICAL_LEVELS, GRID_COLS), jnp.float32) ** shard_levels(streams_of[0], (GRID_ROWS, DEPTH_CLASSES * VERTICAL_LEVELS, GRID_COLS), ((0, 4), (2, 8)), -0.2, 0.2), -20.0, -2.0)
    ice_depth_per_class = jnp.clip(jnp.exp(math.log(3.0) - 1.7917595 * jax.random.uniform(streams_of[1], (GRID_ROWS, DEPTH_CLASSES, GRID_COLS), jnp.float32) ** shard_levels(streams_of[1], (GRID_ROWS, DEPTH_CLASSES, GRID_COLS), ((0, 4), (2, 8)), -0.2, 0.2)), 0.5, 3.0)
    ice_area = jnp.clip(jnp.exp(math.log(0.2) - 1.3862944 * jax.random.uniform(streams_of[2], (GRID_ROWS, DEPTH_CLASSES, GRID_COLS), jnp.float32) ** shard_levels(streams_of[2], (GRID_ROWS, DEPTH_CLASSES, GRID_COLS), ((0, 4), (2, 8)), -0.2, 0.2)), 0.05, 0.2)
    surf_temp = jnp.clip(-30.0 + 28.0 * jax.random.uniform(streams_of[3], (GRID_ROWS, GRID_COLS), jnp.float32) ** shard_levels(streams_of[3], (GRID_ROWS, GRID_COLS), ((0, 4), (1, 8)), -0.2, 0.2), -30.0, -2.0)
    seawater_thermal_input = jnp.clip(0.3 * jax.random.uniform(streams_of[4], (GRID_ROWS, GRID_COLS), jnp.float32) ** shard_levels(streams_of[4], (GRID_ROWS, GRID_COLS), ((0, 4), (1, 8)), -0.2, 0.2), 0.0, 0.3)
    velocity = gaussian(streams_of[5], (2, GRID_ROWS, GRID_COLS), 0.2, 1.2, ((1, 4), (2, 8)), jnp.float32)
    stress = gaussian(streams_of[6], (3, GRID_ROWS, GRID_COLS), 0.5, 3.0, ((1, 4), (2, 8)), jnp.float32)
    wind_stress = gaussian(streams_of[7], (2, GRID_ROWS, GRID_COLS), 0.3, 1.8, ((1, 4), (2, 8)), jnp.float32)
    current = gaussian(streams_of[8], (2, GRID_ROWS, GRID_COLS), 0.3, 1.8, ((1, 4), (2, 8)), jnp.float32)
    land_mask = place_ends((jax.random.randint(streams_of[9], (GRID_ROWS, GRID_COLS), 0, 10) < 9).astype(jnp.int32), jax.random.fold_in(streams_of[9], 1), 0, 1)
    ice_mask = draw_ice_mask(jax.random.fold_in(streams_of[12], 71), 0)
    band_index = draw_band_index(jax.random.fold_in(streams_of[12], 71), 0)
    return dict(layer_temp=layer_temp, ice_depth_per_class=ice_depth_per_class, ice_area=ice_area, surf_temp=surf_temp, seawater_thermal_input=seawater_thermal_input, velocity=velocity, stress=stress, wind_stress=wind_stress, current=current, land_mask=land_mask, ice_mask=ice_mask, band_index=band_index)


FREEZE_POINT = -1.8
BASE_CONDUCT = 2.03
SALT_CONDUCT = 0.416
CONDUCT_SCALE = 1.0
GROWTH_RATE = 0.02
STRENGTH_SCALE = 1.0
STRENGTH_DECAY = 5.0
ELLIPSE_SQUARE = 4.0
STRAIN_FLOOR = 0.0025
STRESS_RELAX = 0.5
MOMENTUM_STEP = 0.5
WATER_DRAG = 1.0

def update_vertical_cell(thermal_state_levels, ice_depth_per_class, upper_interface_state, seawater_thermal_input):
    first_extent = thermal_state_levels.shape[:-2]
    vertical_cell_group = thermal_state_levels.shape[-1]
    vertical_levels_state = thermal_state_levels.reshape(first_extent + (DEPTH_CLASSES, VERTICAL_LEVELS, vertical_cell_group))
    before = [vertical_levels_state[..., layer_at, :] for layer_at in range(VERTICAL_LEVELS)]
    surface_row = upper_interface_state[..., None, :]
    scaled = CONDUCT_SCALE / (ice_depth_per_class * ice_depth_per_class)
    repeated_pass = before
    for picard_turn in range(SWEEPS):
        conductance = [BASE_CONDUCT + SALT_CONDUCT / guessed for guessed in repeated_pass]
        couplings = [scaled * conductance[0]]
        for layer_at in range(1, VERTICAL_LEVELS):
            couplings.append(scaled * 0.5 * (conductance[layer_at - 1] + conductance[layer_at]))
        couplings.append(scaled * conductance[VERTICAL_LEVELS - 1])
        upper_ratio = []
        eliminated = []
        for layer_at in range(VERTICAL_LEVELS):
            source_term = before[layer_at]
            divisor = 1.0 + couplings[layer_at] + couplings[layer_at + 1]
            if layer_at == 0:
                source_term = source_term + couplings[0] * surface_row
            else:
                divisor = divisor - couplings[layer_at] * upper_ratio[layer_at - 1]
                source_term = source_term + couplings[layer_at] * eliminated[layer_at - 1]
            if layer_at == VERTICAL_LEVELS - 1:
                source_term = source_term + couplings[VERTICAL_LEVELS] * FREEZE_POINT
            upper_ratio.append(couplings[layer_at + 1] / divisor)
            eliminated.append(source_term / divisor)
        solved = list(eliminated)
        for layer_at in range(VERTICAL_LEVELS - 2, -1, -1):
            solved[layer_at] = eliminated[layer_at] + upper_ratio[layer_at] * solved[layer_at + 1]
        repeated_pass = solved
    bottom = repeated_pass[VERTICAL_LEVELS - 1]
    regrown = ice_depth_per_class + GROWTH_RATE * (BASE_CONDUCT + SALT_CONDUCT / bottom) * (FREEZE_POINT - bottom) / ice_depth_per_class - seawater_thermal_input[..., None, :]
    updated_vertical_cells = jnp.stack(repeated_pass, axis=-2).reshape(thermal_state_levels.shape)
    return (updated_vertical_cells, regrown)

def pad_rim(field, margin):
    wrapped = jnp.concatenate([field[..., -margin:], field, field[..., :margin]], axis=-1)
    spacing = [(0, 0)] * (field.ndim - 2) + [(margin, margin), (0, 0)]
    return jnp.pad(wrapped, spacing)

def stress_update(zonal_field, meridional_field, previous, strength):
    zonal_east = (zonal_field[1:-1, 2:] - zonal_field[1:-1, :-2]) * 0.5
    zonal_north = (zonal_field[2:, 1:-1] - zonal_field[:-2, 1:-1]) * 0.5
    meridional_east = (meridional_field[1:-1, 2:] - meridional_field[1:-1, :-2]) * 0.5
    meridional_north = (meridional_field[2:, 1:-1] - meridional_field[:-2, 1:-1]) * 0.5
    divergence = zonal_east + meridional_north
    tension = zonal_east - meridional_north
    shearing = zonal_north + meridional_east
    deformation = jnp.sqrt(divergence * divergence + (tension * tension + shearing * shearing) / ELLIPSE_SQUARE + STRAIN_FLOOR)
    viscous = strength / deformation
    bulk_new = (previous[0] + STRESS_RELAX * viscous * (divergence - deformation)) / (1.0 + STRESS_RELAX)
    tension_new = (previous[1] + STRESS_RELAX * viscous * tension / ELLIPSE_SQUARE) / (1.0 + STRESS_RELAX)
    shear_new = (previous[2] + STRESS_RELAX * viscous * shearing / (2.0 * ELLIPSE_SQUARE)) / (1.0 + STRESS_RELAX)
    return jnp.stack([bulk_new, tension_new, shear_new])

def force_update(padded, velocity, ice_mass, wind_stress, current, wet_cells):
    normal_east = 0.5 * (padded[0] + padded[1])
    normal_north = 0.5 * (padded[0] - padded[1])
    shear_stress = padded[2]
    push_east = (normal_east[1:-1, 2:] - normal_east[1:-1, :-2]) * 0.5 + (shear_stress[2:, 1:-1] - shear_stress[:-2, 1:-1]) * 0.5
    push_north = (shear_stress[1:-1, 2:] - shear_stress[1:-1, :-2]) * 0.5 + (normal_north[2:, 1:-1] - normal_north[:-2, 1:-1]) * 0.5
    pushes = jnp.stack([push_east, push_north])
    moved = velocity + MOMENTUM_STEP * (pushes / ice_mass + wind_stress + WATER_DRAG * current)
    return wet_cells * moved / (1.0 + MOMENTUM_STEP * WATER_DRAG)

def one_block(pieces):
    return update_vertical_cell(pieces[0], pieces[1], pieces[2], pieces[3])

def reference(layer_temp, ice_depth_per_class, ice_area, surf_temp, seawater_thermal_input, velocity, stress, wind_stress, current, land_mask, ice_mask, band_index):
    strip_ice = jnp.repeat(jnp.transpose(ice_mask), COLS_DEV, axis=1) == 1
    blocks = (layer_temp.reshape(N_LAT, ROWS_DEV, DEPTH_CLASSES * VERTICAL_LEVELS, GRID_COLS), ice_depth_per_class.reshape(N_LAT, ROWS_DEV, DEPTH_CLASSES, GRID_COLS), surf_temp.reshape(N_LAT, ROWS_DEV, GRID_COLS), seawater_thermal_input.reshape(N_LAT, ROWS_DEV, GRID_COLS))
    stepped_temp, stepped_thick = lax.map(one_block, blocks)
    stepped_temp = stepped_temp.reshape(layer_temp.shape)
    stepped_thick = stepped_thick.reshape(ice_depth_per_class.shape)
    temp_after = jnp.where(strip_ice[:, None, :], stepped_temp, layer_temp)
    thick_after = jnp.where(strip_ice[:, None, :], stepped_thick, ice_depth_per_class)
    volume_start = lax.optimization_barrier(jnp.sum(ice_area * ice_depth_per_class, axis=1))
    coverage = lax.optimization_barrier(jnp.sum(ice_area, axis=1))
    strength = STRENGTH_SCALE * volume_start * jnp.exp(-STRENGTH_DECAY * (1.0 - coverage))
    ice_mass = 1.0 + volume_start
    wet_cells = land_mask.astype(jnp.float32)
    moving = velocity
    stresses = stress
    for subcycle in range(SUBCYCLES):
        padded_velocity = pad_rim(moving, 1)
        stresses = stress_update(padded_velocity[0], padded_velocity[1], stresses, strength)
        moving = force_update(pad_rim(stresses, 1), moving, ice_mass, wind_stress, current, wet_cells)
    volume_after = lax.optimization_barrier(jnp.sum(ice_area * thick_after, axis=1))
    row_total = lax.optimization_barrier(jnp.sum(volume_after, axis=1))
    members = (band_index[:, None] == jnp.arange(BANDS, dtype=jnp.int32)[None, :]).astype(jnp.float32)
    band_sum = lax.optimization_barrier(jnp.sum(members * row_total[:, None], axis=0))
    band_cells = lax.optimization_barrier(jnp.sum(members, axis=0)) * GRID_COLS
    zonal_volume = band_sum / band_cells
    return (temp_after, thick_after, moving, stresses, zonal_volume)
```

```python
import functools

import jax
import jax.numpy as jnp
from jax import lax
from jax.experimental import pallas as pl
from jax.experimental.pallas import tpu as pltpu
from jax.sharding import PartitionSpec as P

DEPTH_CLASSES = 5
VERTICAL_LEVELS = 7
SUBCYCLES = 3
SWEEPS = 2
BANDS_DEV = 4

FREEZE_POINT = -1.8
BASE_CONDUCT = 2.03
SALT_CONDUCT = 0.416
GROWTH_RATE = 0.02
STRENGTH_DECAY = 5.0
ELLIPSE_SQUARE = 4.0
STRAIN_FLOOR = 0.0025
STRESS_RELAX = 0.5
MOMENTUM_STEP = 0.5
WATER_DRAG = 1.0

HALO = 2 * SUBCYCLES
EDGE = 8
FIELDS = 10
EARLY_CLASSES = 1

MESH = pl.DeviceIdType.MESH


def step_columns(temps, depth, surface, seawater):
    inverse = 1.0 / depth
    scaled = inverse * inverse
    half = 0.5 * scaled
    guess = temps
    for turn in range(SWEEPS):
        conduct = [BASE_CONDUCT + SALT_CONDUCT / g for g in guess]
        coupling = [scaled * conduct[0]]
        for k in range(1, VERTICAL_LEVELS):
            coupling.append(half * (conduct[k - 1] + conduct[k]))
        coupling.append(scaled * conduct[-1])
        ratio, done = [], []
        for k in range(VERTICAL_LEVELS):
            source = temps[k]
            divisor = 1.0 + coupling[k] + coupling[k + 1]
            if k == 0:
                source = source + coupling[0] * surface
            else:
                divisor = divisor - coupling[k] * ratio[k - 1]
                source = source + coupling[k] * done[k - 1]
            if k == VERTICAL_LEVELS - 1:
                source = source + coupling[k + 1] * FREEZE_POINT
            scale = 1.0 / divisor
            if k < VERTICAL_LEVELS - 1:
                ratio.append(coupling[k + 1] * scale)
            done.append(source * scale)
        solved = list(done)
        for k in range(VERTICAL_LEVELS - 2, -1, -1):
            solved[k] = done[k] + ratio[k] * solved[k + 1]
        guess = solved
    bottom = guess[-1]
    thick = (
        depth
        + GROWTH_RATE * (BASE_CONDUCT + SALT_CONDUCT / bottom) * (FREEZE_POINT - bottom) * inverse
        - seawater
    )
    return guess, thick


def subcycle(u, v, s1, s2, s12, strength, keep, push_scale, force_x, force_y):
    rows, cols = u.shape

    def dx(f):
        return pltpu.roll(f, cols - 1, 1) - pltpu.roll(f, 1, 1)

    def dy(f):
        return pltpu.roll(f, rows - 1, 0) - pltpu.roll(f, 1, 0)

    ux, vy, uy, vx = dx(u), dy(v), dy(u), dx(v)
    divergence = 0.5 * (ux + vy)
    tension = 0.5 * (ux - vy)
    shearing = 0.5 * (uy + vx)
    deformation = jnp.sqrt(
        divergence * divergence
        + (tension * tension + shearing * shearing) * (1.0 / ELLIPSE_SQUARE)
        + STRAIN_FLOOR
    )
    relax = 1.0 / (1.0 + STRESS_RELAX)
    viscous = (STRESS_RELAX * relax) * strength / deformation
    s1 = relax * s1 + viscous * (divergence - deformation)
    s2 = relax * s2 + viscous * tension * (1.0 / ELLIPSE_SQUARE)
    s12 = relax * s12 + viscous * shearing * (0.5 / ELLIPSE_SQUARE)
    push_x = dx(0.5 * (s1 + s2)) + dy(s12)
    push_y = dx(s12) + dy(0.5 * (s1 - s2))
    u = keep * u + push_scale * push_x + force_x
    v = keep * v + push_scale * push_y + force_y
    return u, v, s1, s2, s12


def as_column(row, rows):
    shape = (rows, rows)
    pick = lax.broadcasted_iota(jnp.int32, shape, 0) == lax.broadcasted_iota(jnp.int32, shape, 1)
    wide = jnp.broadcast_to(row.astype(jnp.float32), shape)
    return jnp.sum(jnp.where(pick, wide, 0.0), axis=1, keepdims=True)


def kernel(n_lat, n_lon, *refs):
    inputs, outputs, scratch = refs[:12], refs[12:17], refs[17:]
    temp_out, thick_out, vel_out, stress_out, zonal_out = outputs
    held = scratch[:12]
    (own, packed, from_up, from_down, from_west, from_east, lat_parts, lon_parts) = scratch[12:20]
    (in_sem, halo_send, halo_recv, lat_send, lat_recv, lon_send, lon_recv) = scratch[20:]
    (temp_in, depth_in, area_in, surf_in, sea_in, vel_in, stress_in) = held[:7]
    (wind_in, current_in, land_in, ice_in, band_in) = held[7:]
    rows, cols = surf_in.shape
    lat, lon = lax.axis_index("lat"), lax.axis_index("lon")
    lats = [lax.rem(lat + d, n_lat) for d in range(n_lat)]
    lons = [lax.rem(lon + d, n_lon) for d in range(n_lon)]
    south, north, east, west = lats[1], lats[-1], lons[1], lons[-1]

    order = (1, 2, 5, 6, 7, 8, 9, 0, 3, 4, 10, 11)
    loads = [pltpu.make_async_copy(inputs[i], held[i], in_sem.at[i]) for i in range(12)]
    for i in order:
        loads[i].start()

    barrier = pltpu.get_barrier_semaphore()
    partners = [(lat, g) for g in lons[1:]] + [(a, lon) for a in lats[1:]]
    partners += [(a, g) for a in (north, south) for g in (west, east)]
    for partner in partners:
        pl.semaphore_signal(barrier, inc=1, device_id=partner, device_id_type=MESH)

    for i in (1, 2, 5, 6, 7, 8, 9):
        loads[i].wait()
    volume = area_in[:, 0, :] * depth_in[:, 0, :]
    coverage = area_in[:, 0, :]
    for c in range(1, DEPTH_CLASSES):
        volume = volume + area_in[:, c, :] * depth_in[:, c, :]
        coverage = coverage + area_in[:, c, :]
    strength = volume * jnp.exp(-STRENGTH_DECAY * (1.0 - coverage))
    drag = 1.0 / (1.0 + MOMENTUM_STEP * WATER_DRAG)
    keep = land_in[...].astype(jnp.float32) * drag
    forced = MOMENTUM_STEP * keep
    push_scale = 0.5 * forced / (1.0 + volume)
    fields = [vel_in[0], vel_in[1], stress_in[0], stress_in[1], stress_in[2], strength, keep]
    fields += [push_scale]
    fields += [forced * (wind_in[i] + WATER_DRAG * current_in[i]) for i in range(2)]
    lane = lax.broadcasted_iota(jnp.int32, (rows, cols), 1)
    pack = jnp.zeros((rows, cols), jnp.float32)
    for f in range(FIELDS):
        first = 2 * HALO * f
        turned = pltpu.roll(fields[f], (first + HALO) % cols, 1)
        pack = jnp.where((lane >= first) & (lane < first + 2 * HALO), turned, pack)
    packed[...] = pack
    for f in range(FIELDS):
        own[f] = fields[f]

    for i in (0, 3, 4, 10, 11):
        loads[i].wait()
    surface, seawater = surf_in[...], sea_in[...]
    icy = as_column(ice_in[...], rows) == 1.0

    def thermo(c):
        first = c * VERTICAL_LEVELS
        temps = [temp_in[:, first + k, :] for k in range(VERTICAL_LEVELS)]
        depth = depth_in[:, c, :]
        stepped, thick = step_columns(temps, depth, surface, seawater)
        thick = jnp.where(icy, thick, depth)
        for k in range(VERTICAL_LEVELS):
            temp_out[:, first + k, :] = jnp.where(icy, stepped[k], temps[k])
        thick_out[:, c, :] = thick
        return area_in[:, c, :] * thick

    after = jnp.zeros((rows, cols), jnp.float32)
    for c in range(EARLY_CLASSES):
        after = after + thermo(c)

    pl.semaphore_wait(barrier, len(partners))

    tail, head = pl.ds(rows - EDGE, EDGE), pl.ds(0, EDGE)
    above, middle, below = pl.ds(0, EDGE), pl.ds(EDGE, rows), pl.ds(EDGE + rows, EDGE)
    plan = (
        (packed.at[tail], from_west.at[above], (south, east)),
        (packed.at[tail], from_east.at[above], (south, west)),
        (packed.at[head], from_west.at[below], (north, east)),
        (packed.at[head], from_east.at[below], (north, west)),
        (packed, from_west.at[middle], (lat, east)),
        (packed, from_east.at[middle], (lat, west)),
        (own.at[:, tail], from_up, (south, lon)),
        (own.at[:, head], from_down, (north, lon)),
    )
    halos = [
        pltpu.make_async_remote_copy(
            src_ref=source,
            dst_ref=target,
            send_sem=halo_send.at[i],
            recv_sem=halo_recv.at[i],
            device_id=device,
            device_id_type=MESH,
        )
        for i, (source, target, device) in enumerate(plan)
    ]
    for copy in halos:
        copy.start()

    for c in range(EARLY_CLASSES, DEPTH_CLASSES):
        after = after + thermo(c)
    total = jnp.sum(after, axis=1, keepdims=True)
    width = lat_parts.shape[-1]
    member = as_column(band_in[...], rows).astype(jnp.int32) == lax.broadcasted_iota(
        jnp.int32, (rows, width), 1
    )
    sums = jnp.sum(jnp.where(member, total, 0.0), axis=0, keepdims=True)
    cells = jnp.sum(jnp.where(member, float(cols), 0.0), axis=0, keepdims=True)
    top = lax.broadcasted_iota(jnp.int32, (EDGE, width), 0) == 0
    lat_parts[lat] = jnp.where(top, sums, cells)

    def share(parts, here, send_sem, recv_sem, devices):
        copies = [
            pltpu.make_async_remote_copy(
                src_ref=parts.at[here],
                dst_ref=parts.at[here],
                send_sem=send_sem.at[d],
                recv_sem=recv_sem.at[d],
                device_id=device,
                device_id_type=MESH,
            )
            for d, device in enumerate(devices)
        ]
        for copy in copies:
            copy.start()
        return copies

    lat_copies = share(lat_parts, lat, lat_send, lat_recv, [(a, lon) for a in lats[1:]])
    for copy in lat_copies:
        copy.wait_recv()
    lon_parts[lon] = jnp.sum(lat_parts[...], axis=0)
    lon_copies = share(lon_parts, lon, lon_send, lon_recv, [(lat, g) for g in lons[1:]])

    for copy in halos:
        copy.wait_recv()
    tall = rows + 2 * EDGE
    place = lax.broadcasted_iota(jnp.int32, (tall, cols), 1)
    merged = jnp.where(lax.rem(place, 2 * HALO) < HALO, from_west[...], from_east[...])
    low = jnp.where(lat == 0, EDGE, 0)
    high = jnp.where(lat == n_lat - 1, EDGE + rows, tall)
    row_id = lax.broadcasted_iota(jnp.int32, (tall, 2 * cols), 0)
    inside = (row_id >= low) & (row_id < high)
    state = []
    for f in range(FIELDS):
        centre = jnp.concatenate([from_up[f], own[f], from_down[f]], axis=0)
        sides = pltpu.roll(merged, (cols - 2 * HALO * f - HALO) % cols, 1)
        state.append(jnp.where(inside, jnp.concatenate([centre, sides], axis=1), 0.0))
    moving, fixed = state[:5], state[5:]
    for turn in range(SUBCYCLES):
        moving = subcycle(*moving, *fixed)
    for i in range(2):
        vel_out[i] = moving[i][EDGE : EDGE + rows, :cols]
    for i in range(3):
        stress_out[i] = moving[2 + i][EDGE : EDGE + rows, :cols]

    for copy in lon_copies:
        copy.wait_recv()
    zonal_out[...] = jnp.sum(lon_parts[...], axis=0)
    for copy in halos + lat_copies + lon_copies:
        copy.wait_send()


def local(n_lat, n_lon, *args):
    args = list(args)
    args[11] = args[11].reshape(1, -1)
    rows, cols = args[3].shape
    bands = BANDS_DEV * n_lat
    width = -(-bands // cols) * cols
    tall = rows + 2 * EDGE
    f32 = jnp.float32
    vmem = pl.BlockSpec(memory_space=pltpu.VMEM)
    outs = [jax.ShapeDtypeStruct(args[i].shape, f32) for i in (0, 1, 5, 6)]
    outs.append(jax.ShapeDtypeStruct((EDGE, width), f32))
    dma = pltpu.SemaphoreType.DMA
    temp, thick, vel, stress, zonal = pl.pallas_call(
        functools.partial(kernel, n_lat, n_lon),
        out_shape=outs,
        in_specs=[pl.BlockSpec(memory_space=pl.ANY)] * 12,
        out_specs=[vmem] * 5,
        scratch_shapes=[pltpu.VMEM(a.shape, a.dtype) for a in args]
        + [
            pltpu.VMEM((FIELDS, rows, cols), f32),
            pltpu.VMEM((rows, cols), f32),
            pltpu.VMEM((FIELDS, EDGE, cols), f32),
            pltpu.VMEM((FIELDS, EDGE, cols), f32),
            pltpu.VMEM((tall, cols), f32),
            pltpu.VMEM((tall, cols), f32),
            pltpu.VMEM((n_lat, EDGE, width), f32),
            pltpu.VMEM((n_lon, EDGE, width), f32),
            dma((12,)),
            dma((8,)),
            dma((8,)),
            dma((n_lat - 1,)),
            dma((n_lat - 1,)),
            dma((n_lon - 1,)),
            dma((n_lon - 1,)),
        ],
        compiler_params=pltpu.CompilerParams(collective_id=0, has_side_effects=True),
        name="ice_step",
    )(*args)
    start = lax.axis_index("lat") * BANDS_DEV
    mine = lax.dynamic_slice_in_dim(zonal, start, BANDS_DEV, axis=1)
    return (temp, thick, vel, stress, mine[0] / mine[1])


def solution(mesh):
    shape = dict(mesh.shape)
    return jax.shard_map(
        functools.partial(local, shape["lat"], shape["lon"]),
        mesh=mesh,
        in_specs=(
            P("lat", None, "lon"),
            P("lat", None, "lon"),
            P("lat", None, "lon"),
            P("lat", "lon"),
            P("lat", "lon"),
            P(None, "lat", "lon"),
            P(None, "lat", "lon"),
            P(None, "lat", "lon"),
            P(None, "lat", "lon"),
            P("lat", "lon"),
            P("lon", "lat"),
            P("lat"),
        ),
        out_specs=(
            P("lat", None, "lon"),
            P("lat", None, "lon"),
            P(None, "lat", "lon"),
            P(None, "lat", "lon"),
            P("lat"),
        ),
        check_vma=False,
    )
```

```python
import functools

import jax
import jax.numpy as jnp
from jax import lax
from jax.experimental import pallas as pl
from jax.experimental.pallas import tpu as pltpu
from jax.sharding import PartitionSpec as P

DEPTH_CLASSES = 5
VERTICAL_LEVELS = 7
SUBCYCLES = 3
SWEEPS = 2
BANDS_DEV = 4

FREEZE_POINT = -1.8
BASE_CONDUCT = 2.03
SALT_CONDUCT = 0.416
GROWTH_RATE = 0.02
STRENGTH_DECAY = 5.0
ELLIPSE_SQUARE = 4.0
STRAIN_FLOOR = 0.0025
STRESS_RELAX = 0.5
MOMENTUM_STEP = 0.5
WATER_DRAG = 1.0

HALO = 2 * SUBCYCLES
EDGE = 8
FIELDS = 10
EARLY_CLASSES = 1

MESH = pl.DeviceIdType.MESH


def step_columns(temps, depth, surface, seawater):
    inverse = 1.0 / depth
    scaled = inverse * inverse
    half = 0.5 * scaled
    guess = temps
    for turn in range(SWEEPS):
        conduct = [BASE_CONDUCT + SALT_CONDUCT / g for g in guess]
        coupling = [scaled * conduct[0]]
        for k in range(1, VERTICAL_LEVELS):
            coupling.append(half * (conduct[k - 1] + conduct[k]))
        coupling.append(scaled * conduct[-1])
        ratio, done = [], []
        for k in range(VERTICAL_LEVELS):
            source = temps[k]
            divisor = 1.0 + coupling[k] + coupling[k + 1]
            if k == 0:
                source = source + coupling[0] * surface
            else:
                divisor = divisor - coupling[k] * ratio[k - 1]
                source = source + coupling[k] * done[k - 1]
            if k == VERTICAL_LEVELS - 1:
                source = source + coupling[k + 1] * FREEZE_POINT
            scale = 1.0 / divisor
            if k < VERTICAL_LEVELS - 1:
                ratio.append(coupling[k + 1] * scale)
            done.append(source * scale)
        solved = list(done)
        for k in range(VERTICAL_LEVELS - 2, -1, -1):
            solved[k] = done[k] + ratio[k] * solved[k + 1]
        guess = solved
    bottom = guess[-1]
    thick = (
        depth
        + GROWTH_RATE * (BASE_CONDUCT + SALT_CONDUCT / bottom) * (FREEZE_POINT - bottom) * inverse
        - seawater
    )
    return guess, thick


def subcycle(u, v, s1, s2, s12, strength, keep, push_scale, force_x, force_y):
    rows, cols = u.shape

    def dx(f):
        return pltpu.roll(f, cols - 1, 1) - pltpu.roll(f, 1, 1)

    def dy(f):
        return pltpu.roll(f, rows - 1, 0) - pltpu.roll(f, 1, 0)

    ux, vy, uy, vx = dx(u), dy(v), dy(u), dx(v)
    divergence = 0.5 * (ux + vy)
    tension = 0.5 * (ux - vy)
    shearing = 0.5 * (uy + vx)
    deformation = jnp.sqrt(
        divergence * divergence
        + (tension * tension + shearing * shearing) * (1.0 / ELLIPSE_SQUARE)
        + STRAIN_FLOOR
    )
    relax = 1.0 / (1.0 + STRESS_RELAX)
    viscous = (STRESS_RELAX * relax) * strength / deformation
    s1 = relax * s1 + viscous * (divergence - deformation)
    s2 = relax * s2 + viscous * tension * (1.0 / ELLIPSE_SQUARE)
    s12 = relax * s12 + viscous * shearing * (0.5 / ELLIPSE_SQUARE)
    push_x = dx(0.5 * (s1 + s2)) + dy(s12)
    push_y = dx(s12) + dy(0.5 * (s1 - s2))
    u = keep * u + push_scale * push_x + force_x
    v = keep * v + push_scale * push_y + force_y
    return u, v, s1, s2, s12


def as_column(row, rows):
    shape = (rows, rows)
    pick = lax.broadcasted_iota(jnp.int32, shape, 0) == lax.broadcasted_iota(jnp.int32, shape, 1)
    wide = jnp.broadcast_to(row.astype(jnp.float32), shape)
    return jnp.sum(jnp.where(pick, wide, 0.0), axis=1, keepdims=True)


def kernel(n_lat, n_lon, *refs):
    inputs, outputs, scratch = refs[:12], refs[12:17], refs[17:]
    temp_out, thick_out, vel_out, stress_out, zonal_out = outputs
    held = scratch[:12]
    (own, packed, from_up, from_down, from_west, from_east, lat_parts, lon_parts) = scratch[12:20]
    (in_sem, halo_send, halo_recv, lat_send, lat_recv, lon_send, lon_recv) = scratch[20:]
    (temp_in, depth_in, area_in, surf_in, sea_in, vel_in, stress_in) = held[:7]
    (wind_in, current_in, land_in, ice_in, band_in) = held[7:]
    rows, cols = surf_in.shape
    lat, lon = lax.axis_index("lat"), lax.axis_index("lon")
    lats = [lax.rem(lat + d, n_lat) for d in range(n_lat)]
    lons = [lax.rem(lon + d, n_lon) for d in range(n_lon)]
    south, north, east, west = lats[1], lats[-1], lons[1], lons[-1]

    order = (1, 2, 5, 6, 7, 8, 9, 0, 3, 4, 10, 11)
    loads = [pltpu.make_async_copy(inputs[i], held[i], in_sem.at[i]) for i in range(12)]
    for i in order:
        loads[i].start()

    barrier = pltpu.get_barrier_semaphore()
    partners = [(lat, g) for g in lons[1:]] + [(a, lon) for a in lats[1:]]
    partners += [(a, g) for a in (north, south) for g in (west, east)]
    for partner in partners:
        pl.semaphore_signal(barrier, inc=1, device_id=partner, device_id_type=MESH)

    for i in (1, 2, 5, 6, 7, 8, 9):
        loads[i].wait()
    volume = area_in[0] * depth_in[0]
    coverage = area_in[0]
    for c in range(1, DEPTH_CLASSES):
        volume = volume + area_in[c] * depth_in[c]
        coverage = coverage + area_in[c]
    strength = volume * jnp.exp(-STRENGTH_DECAY * (1.0 - coverage))
    drag = 1.0 / (1.0 + MOMENTUM_STEP * WATER_DRAG)
    keep = land_in[...].astype(jnp.float32) * drag
    forced = MOMENTUM_STEP * keep
    push_scale = 0.5 * forced / (1.0 + volume)
    fields = [vel_in[0], vel_in[1], stress_in[0], stress_in[1], stress_in[2], strength, keep]
    fields += [push_scale]
    fields += [forced * (wind_in[i] + WATER_DRAG * current_in[i]) for i in range(2)]
    lane = lax.broadcasted_iota(jnp.int32, (rows, cols), 1)
    pack = jnp.zeros((rows, cols), jnp.float32)
    for f in range(FIELDS):
        first = 2 * HALO * f
        turned = pltpu.roll(fields[f], (first + HALO) % cols, 1)
        pack = jnp.where((lane >= first) & (lane < first + 2 * HALO), turned, pack)
    packed[...] = pack
    for f in range(FIELDS):
        own[f] = fields[f]

    for i in (0, 3, 4, 10, 11):
        loads[i].wait()
    surface, seawater = surf_in[...], sea_in[...]
    icy = as_column(ice_in[...], rows) == 1.0

    def thermo(c):
        first = c * VERTICAL_LEVELS
        temps = [temp_in[first + k] for k in range(VERTICAL_LEVELS)]
        depth = depth_in[c]
        stepped, thick = step_columns(temps, depth, surface, seawater)
        thick = jnp.where(icy, thick, depth)
        for k in range(VERTICAL_LEVELS):
            temp_out[first + k] = jnp.where(icy, stepped[k], temps[k])
        thick_out[c] = thick
        return area_in[c] * thick

    after = jnp.zeros((rows, cols), jnp.float32)
    for c in range(EARLY_CLASSES):
        after = after + thermo(c)

    pl.semaphore_wait(barrier, len(partners))

    tail, head = pl.ds(rows - EDGE, EDGE), pl.ds(0, EDGE)
    above, middle, below = pl.ds(0, EDGE), pl.ds(EDGE, rows), pl.ds(EDGE + rows, EDGE)
    plan = (
        (packed.at[tail], from_west.at[above], (south, east)),
        (packed.at[tail], from_east.at[above], (south, west)),
        (packed.at[head], from_west.at[below], (north, east)),
        (packed.at[head], from_east.at[below], (north, west)),
        (packed, from_west.at[middle], (lat, east)),
        (packed, from_east.at[middle], (lat, west)),
        (own.at[:, tail], from_up, (south, lon)),
        (own.at[:, head], from_down, (north, lon)),
    )
    halos = [
        pltpu.make_async_remote_copy(
            src_ref=source,
            dst_ref=target,
            send_sem=halo_send.at[i],
            recv_sem=halo_recv.at[i],
            device_id=device,
            device_id_type=MESH,
        )
        for i, (source, target, device) in enumerate(plan)
    ]
    for copy in halos:
        copy.start()

    for c in range(EARLY_CLASSES, DEPTH_CLASSES):
        after = after + thermo(c)
    total = jnp.sum(after, axis=1, keepdims=True)
    width = lat_parts.shape[-1]
    member = as_column(band_in[...], rows).astype(jnp.int32) == lax.broadcasted_iota(
        jnp.int32, (rows, width), 1
    )
    sums = jnp.sum(jnp.where(member, total, 0.0), axis=0, keepdims=True)
    cells = jnp.sum(jnp.where(member, float(cols), 0.0), axis=0, keepdims=True)
    top = lax.broadcasted_iota(jnp.int32, (EDGE, width), 0) == 0
    lat_parts[lat] = jnp.where(top, sums, cells)

    def share(parts, here, send_sem, recv_sem, devices):
        copies = [
            pltpu.make_async_remote_copy(
                src_ref=parts.at[here],
                dst_ref=parts.at[here],
                send_sem=send_sem.at[d],
                recv_sem=recv_sem.at[d],
                device_id=device,
                device_id_type=MESH,
            )
            for d, device in enumerate(devices)
        ]
        for copy in copies:
            copy.start()
        return copies

    lat_copies = share(lat_parts, lat, lat_send, lat_recv, [(a, lon) for a in lats[1:]])
    for copy in lat_copies:
        copy.wait_recv()
    lon_parts[lon] = jnp.sum(lat_parts[...], axis=0)
    lon_copies = share(lon_parts, lon, lon_send, lon_recv, [(lat, g) for g in lons[1:]])

    for copy in halos:
        copy.wait_recv()
    tall = rows + 2 * EDGE
    place = lax.broadcasted_iota(jnp.int32, (tall, cols), 1)
    merged = jnp.where(lax.rem(place, 2 * HALO) < HALO, from_west[...], from_east[...])
    low = jnp.where(lat == 0, EDGE, 0)
    high = jnp.where(lat == n_lat - 1, EDGE + rows, tall)
    row_id = lax.broadcasted_iota(jnp.int32, (tall, 2 * cols), 0)
    inside = (row_id >= low) & (row_id < high)
    state = []
    for f in range(FIELDS):
        centre = jnp.concatenate([from_up[f], own[f], from_down[f]], axis=0)
        sides = pltpu.roll(merged, (cols - 2 * HALO * f - HALO) % cols, 1)
        state.append(jnp.where(inside, jnp.concatenate([centre, sides], axis=1), 0.0))
    moving, fixed = state[:5], state[5:]
    for turn in range(SUBCYCLES):
        moving = subcycle(*moving, *fixed)
    for i in range(2):
        vel_out[i] = moving[i][EDGE : EDGE + rows, :cols]
    for i in range(3):
        stress_out[i] = moving[2 + i][EDGE : EDGE + rows, :cols]

    for copy in lon_copies:
        copy.wait_recv()
    whole = jnp.sum(lon_parts[...], axis=0)
    mean = whole[:1] / jnp.maximum(whole[1:2], 1.0)
    mine = jnp.zeros((1, BANDS_DEV), jnp.float32)
    for a in range(n_lat):
        mine = jnp.where(lat == a, mean[:, a * BANDS_DEV : (a + 1) * BANDS_DEV], mine)
    zonal_out[...] = mine
    for copy in halos + lat_copies + lon_copies:
        copy.wait_send()


def put_out(*refs):
    sem = refs[10]
    copies = [pltpu.make_async_copy(refs[i], refs[5 + i], sem.at[i]) for i in range(5)]
    for copy in copies:
        copy.start()
    for copy in copies:
        copy.wait()


def local(n_lat, n_lon, *args):
    args = list(args)
    args[:3] = [jnp.transpose(a, (1, 0, 2)) for a in args[:3]]
    args[11] = args[11].reshape(1, -1)
    rows, cols = args[3].shape
    bands = BANDS_DEV * n_lat
    width = -(-bands // cols) * cols
    tall = rows + 2 * EDGE
    f32 = jnp.float32
    vmem = pl.BlockSpec(memory_space=pltpu.VMEM)
    shapes = [args[i].shape for i in (0, 1, 5, 6)] + [(1, BANDS_DEV)]
    dma = pltpu.SemaphoreType.DMA
    results = pl.pallas_call(
        functools.partial(kernel, n_lat, n_lon),
        out_shape=[pltpu.VMEM(shape, f32) for shape in shapes],
        in_specs=[pl.BlockSpec(memory_space=pl.ANY)] * 12,
        out_specs=[vmem] * 5,
        scratch_shapes=[pltpu.VMEM(a.shape, a.dtype) for a in args]
        + [
            pltpu.VMEM((FIELDS, rows, cols), f32),
            pltpu.VMEM((rows, cols), f32),
            pltpu.VMEM((FIELDS, EDGE, cols), f32),
            pltpu.VMEM((FIELDS, EDGE, cols), f32),
            pltpu.VMEM((tall, cols), f32),
            pltpu.VMEM((tall, cols), f32),
            pltpu.VMEM((n_lat, EDGE, width), f32),
            pltpu.VMEM((n_lon, EDGE, width), f32),
            dma((12,)),
            dma((8,)),
            dma((8,)),
            dma((n_lat - 1,)),
            dma((n_lat - 1,)),
            dma((n_lon - 1,)),
            dma((n_lon - 1,)),
        ],
        compiler_params=pltpu.CompilerParams(collective_id=0, has_side_effects=True),
        name="ice_step",
    )(*args)
    temp, thick, vel, stress, zonal = pl.pallas_call(
        put_out,
        out_shape=[jax.ShapeDtypeStruct(shape, f32) for shape in shapes],
        in_specs=[vmem] * 5,
        out_specs=[pl.BlockSpec(memory_space=pl.ANY)] * 5,
        scratch_shapes=[dma((5,))],
        name="put_out",
    )(*[pltpu.with_memory_space_constraint(r, pltpu.VMEM) for r in results])
    temp, thick = [jnp.transpose(a, (1, 0, 2)) for a in (temp, thick)]
    return (temp, thick, vel, stress, zonal.reshape(BANDS_DEV))


def solution(mesh):
    shape = dict(mesh.shape)
    return jax.shard_map(
        functools.partial(local, shape["lat"], shape["lon"]),
        mesh=mesh,
        in_specs=(
            P("lat", None, "lon"),
            P("lat", None, "lon"),
            P("lat", None, "lon"),
            P("lat", "lon"),
            P("lat", "lon"),
            P(None, "lat", "lon"),
            P(None, "lat", "lon"),
            P(None, "lat", "lon"),
            P(None, "lat", "lon"),
            P("lat", "lon"),
            P("lon", "lat"),
            P("lat"),
        ),
        out_specs=(
            P("lat", None, "lon"),
            P("lat", None, "lon"),
            P(None, "lat", "lon"),
            P(None, "lat", "lon"),
            P("lat"),
        ),
        check_vma=False,
    )
```

```python
import functools

import jax
import jax.numpy as jnp
from jax import lax
from jax.experimental import pallas as pl
from jax.experimental.pallas import tpu as pltpu
from jax.sharding import PartitionSpec as P

DEPTH_CLASSES = 5
VERTICAL_LEVELS = 7
SUBCYCLES = 3
SWEEPS = 2
BANDS_DEV = 4

FREEZE_POINT = -1.8
BASE_CONDUCT = 2.03
SALT_CONDUCT = 0.416
GROWTH_RATE = 0.02
STRENGTH_DECAY = 5.0
ELLIPSE_SQUARE = 4.0
STRAIN_FLOOR = 0.0025
STRESS_RELAX = 0.5
MOMENTUM_STEP = 0.5
WATER_DRAG = 1.0

HALO = 2 * SUBCYCLES
EDGE = 8
FIELDS = 10
EARLY_CLASSES = 2

MESH = pl.DeviceIdType.MESH


def step_columns(temps, depth, surface, seawater):
    inverse = 1.0 / depth
    scaled = inverse * inverse
    half = 0.5 * scaled
    guess = temps
    for turn in range(SWEEPS):
        conduct = [BASE_CONDUCT + SALT_CONDUCT / g for g in guess]
        coupling = [scaled * conduct[0]]
        for k in range(1, VERTICAL_LEVELS):
            coupling.append(half * (conduct[k - 1] + conduct[k]))
        coupling.append(scaled * conduct[-1])
        ratio, done = [], []
        for k in range(VERTICAL_LEVELS):
            source = temps[k]
            divisor = 1.0 + coupling[k] + coupling[k + 1]
            if k == 0:
                source = source + coupling[0] * surface
            else:
                divisor = divisor - coupling[k] * ratio[k - 1]
                source = source + coupling[k] * done[k - 1]
            if k == VERTICAL_LEVELS - 1:
                source = source + coupling[k + 1] * FREEZE_POINT
            scale = 1.0 / divisor
            if k < VERTICAL_LEVELS - 1:
                ratio.append(coupling[k + 1] * scale)
            done.append(source * scale)
        solved = list(done)
        for k in range(VERTICAL_LEVELS - 2, -1, -1):
            solved[k] = done[k] + ratio[k] * solved[k + 1]
        guess = solved
    bottom = guess[-1]
    thick = (
        depth
        + GROWTH_RATE * (BASE_CONDUCT + SALT_CONDUCT / bottom) * (FREEZE_POINT - bottom) * inverse
        - seawater
    )
    return guess, thick


def subcycle(u, v, s1, s2, s12, strength, keep, push_scale, force_x, force_y):
    rows, cols = u.shape

    def dx(f):
        return pltpu.roll(f, cols - 1, 1) - pltpu.roll(f, 1, 1)

    def dy(f):
        return pltpu.roll(f, rows - 1, 0) - pltpu.roll(f, 1, 0)

    ux, vy, uy, vx = dx(u), dy(v), dy(u), dx(v)
    divergence = 0.5 * (ux + vy)
    tension = 0.5 * (ux - vy)
    shearing = 0.5 * (uy + vx)
    deformation = jnp.sqrt(
        divergence * divergence
        + (tension * tension + shearing * shearing) * (1.0 / ELLIPSE_SQUARE)
        + STRAIN_FLOOR
    )
    relax = 1.0 / (1.0 + STRESS_RELAX)
    viscous = (STRESS_RELAX * relax) * strength / deformation
    s1 = relax * s1 + viscous * (divergence - deformation)
    s2 = relax * s2 + viscous * tension * (1.0 / ELLIPSE_SQUARE)
    s12 = relax * s12 + viscous * shearing * (0.5 / ELLIPSE_SQUARE)
    push_x = dx(0.5 * (s1 + s2)) + dy(s12)
    push_y = dx(s12) + dy(0.5 * (s1 - s2))
    u = keep * u + push_scale * push_x + force_x
    v = keep * v + push_scale * push_y + force_y
    return u, v, s1, s2, s12


def as_column(row, rows):
    shape = (rows, rows)
    pick = lax.broadcasted_iota(jnp.int32, shape, 0) == lax.broadcasted_iota(jnp.int32, shape, 1)
    wide = jnp.broadcast_to(row.astype(jnp.float32), shape)
    return jnp.sum(jnp.where(pick, wide, 0.0), axis=1, keepdims=True)


def kernel(n_lat, n_lon, *refs):
    inputs, outputs, scratch = refs[:12], refs[12:17], refs[17:]
    temp_out, thick_out, vel_out, stress_out, zonal_out = outputs
    held = scratch[:12]
    (own, packed, from_up, from_down, from_west, from_east, lat_parts, lon_parts) = scratch[12:20]
    (in_sem, halo_send, halo_recv, lat_send, lat_recv, lon_send, lon_recv) = scratch[20:]
    (temp_in, depth_in, area_in, surf_in, sea_in, vel_in, stress_in) = held[:7]
    (wind_in, current_in, land_in, ice_in, band_in) = held[7:]
    rows, cols = surf_in.shape
    lat, lon = lax.axis_index("lat"), lax.axis_index("lon")
    lats = [lax.rem(lat + d, n_lat) for d in range(n_lat)]
    lons = [lax.rem(lon + d, n_lon) for d in range(n_lon)]
    south, north, east, west = lats[1], lats[-1], lons[1], lons[-1]

    order = (1, 2, 5, 6, 7, 8, 9, 0, 3, 4, 10, 11)
    loads = [pltpu.make_async_copy(inputs[i], held[i], in_sem.at[i]) for i in range(12)]
    for i in order:
        loads[i].start()

    barrier = pltpu.get_barrier_semaphore()
    partners = [(lat, g) for g in lons[1:]] + [(a, lon) for a in lats[1:]]
    partners += [(a, g) for a in (north, south) for g in (west, east)]
    for partner in partners:
        pl.semaphore_signal(barrier, inc=1, device_id=partner, device_id_type=MESH)

    for i in (1, 2, 5, 6, 7, 8, 9):
        loads[i].wait()
    volume = area_in[0] * depth_in[0]
    coverage = area_in[0]
    for c in range(1, DEPTH_CLASSES):
        volume = volume + area_in[c] * depth_in[c]
        coverage = coverage + area_in[c]
    strength = volume * jnp.exp(-STRENGTH_DECAY * (1.0 - coverage))
    drag = 1.0 / (1.0 + MOMENTUM_STEP * WATER_DRAG)
    keep = land_in[...].astype(jnp.float32) * drag
    forced = MOMENTUM_STEP * keep
    push_scale = 0.5 * forced / (1.0 + volume)
    fields = [vel_in[0], vel_in[1], stress_in[0], stress_in[1], stress_in[2], strength, keep]
    fields += [push_scale]
    fields += [forced * (wind_in[i] + WATER_DRAG * current_in[i]) for i in range(2)]
    lane = lax.broadcasted_iota(jnp.int32, (rows, cols), 1)
    pack = jnp.zeros((rows, cols), jnp.float32)
    for f in range(FIELDS):
        first = 2 * HALO * f
        turned = pltpu.roll(fields[f], (first + HALO) % cols, 1)
        pack = jnp.where((lane >= first) & (lane < first + 2 * HALO), turned, pack)
    packed[...] = pack
    for f in range(FIELDS):
        own[f] = fields[f]

    for i in (0, 3, 4, 10, 11):
        loads[i].wait()
    surface, seawater = surf_in[...], sea_in[...]
    icy = as_column(ice_in[...], rows) == 1.0

    def thermo(c):
        first = c * VERTICAL_LEVELS
        temps = [temp_in[first + k] for k in range(VERTICAL_LEVELS)]
        depth = depth_in[c]
        stepped, thick = step_columns(temps, depth, surface, seawater)
        thick = jnp.where(icy, thick, depth)
        for k in range(VERTICAL_LEVELS):
            temp_out[first + k] = jnp.where(icy, stepped[k], temps[k])
        thick_out[c] = thick
        return area_in[c] * thick

    after = jnp.zeros((rows, cols), jnp.float32)
    for c in range(EARLY_CLASSES):
        after = after + thermo(c)

    pl.semaphore_wait(barrier, len(partners))

    tail, head = pl.ds(rows - EDGE, EDGE), pl.ds(0, EDGE)
    above, middle, below = pl.ds(0, EDGE), pl.ds(EDGE, rows), pl.ds(EDGE + rows, EDGE)
    plan = (
        (packed.at[tail], from_west.at[above], (south, east)),
        (packed.at[tail], from_east.at[above], (south, west)),
        (packed.at[head], from_west.at[below], (north, east)),
        (packed.at[head], from_east.at[below], (north, west)),
        (packed, from_west.at[middle], (lat, east)),
        (packed, from_east.at[middle], (lat, west)),
        (own.at[:, tail], from_up, (south, lon)),
        (own.at[:, head], from_down, (north, lon)),
    )
    halos = [
        pltpu.make_async_remote_copy(
            src_ref=source,
            dst_ref=target,
            send_sem=halo_send.at[i],
            recv_sem=halo_recv.at[i],
            device_id=device,
            device_id_type=MESH,
        )
        for i, (source, target, device) in enumerate(plan)
    ]
    for copy in halos:
        copy.start()

    for c in range(EARLY_CLASSES, DEPTH_CLASSES):
        after = after + thermo(c)
    total = jnp.sum(after, axis=1, keepdims=True)
    width = lat_parts.shape[-1]
    member = as_column(band_in[...], rows).astype(jnp.int32) == lax.broadcasted_iota(
        jnp.int32, (rows, width), 1
    )
    sums = jnp.sum(jnp.where(member, total, 0.0), axis=0, keepdims=True)
    cells = jnp.sum(jnp.where(member, float(cols), 0.0), axis=0, keepdims=True)
    top = lax.broadcasted_iota(jnp.int32, (EDGE, width), 0) == 0
    lat_parts[lat] = jnp.where(top, sums, cells)

    def share(parts, here, send_sem, recv_sem, devices):
        copies = [
            pltpu.make_async_remote_copy(
                src_ref=parts.at[here],
                dst_ref=parts.at[here],
                send_sem=send_sem.at[d],
                recv_sem=recv_sem.at[d],
                device_id=device,
                device_id_type=MESH,
            )
            for d, device in enumerate(devices)
        ]
        for copy in copies:
            copy.start()
        return copies

    lat_copies = share(lat_parts, lat, lat_send, lat_recv, [(a, lon) for a in lats[1:]])
    for copy in lat_copies:
        copy.wait_recv()
    lon_parts[lon] = jnp.sum(lat_parts[...], axis=0)
    lon_copies = share(lon_parts, lon, lon_send, lon_recv, [(lat, g) for g in lons[1:]])

    for copy in halos:
        copy.wait_recv()
    tall = rows + 2 * EDGE
    place = lax.broadcasted_iota(jnp.int32, (tall, cols), 1)
    merged = jnp.where(lax.rem(place, 2 * HALO) < HALO, from_west[...], from_east[...])
    low = jnp.where(lat == 0, EDGE, 0)
    high = jnp.where(lat == n_lat - 1, EDGE + rows, tall)
    row_id = lax.broadcasted_iota(jnp.int32, (tall, 2 * cols), 0)
    inside = (row_id >= low) & (row_id < high)
    state = []
    for f in range(FIELDS):
        centre = jnp.concatenate([from_up[f], own[f], from_down[f]], axis=0)
        sides = pltpu.roll(merged, (cols - 2 * HALO * f - HALO) % cols, 1)
        state.append(jnp.where(inside, jnp.concatenate([centre, sides], axis=1), 0.0))
    moving, fixed = state[:5], state[5:]
    for turn in range(SUBCYCLES):
        moving = subcycle(*moving, *fixed)
    for i in range(2):
        vel_out[i] = moving[i][EDGE : EDGE + rows, :cols]
    for i in range(3):
        stress_out[i] = moving[2 + i][EDGE : EDGE + rows, :cols]

    for copy in lon_copies:
        copy.wait_recv()
    whole = jnp.sum(lon_parts[...], axis=0)
    mean = whole[:1] / jnp.maximum(whole[1:2], 1.0)
    mine = jnp.zeros((1, BANDS_DEV), jnp.float32)
    for a in range(n_lat):
        mine = jnp.where(lat == a, mean[:, a * BANDS_DEV : (a + 1) * BANDS_DEV], mine)
    zonal_out[...] = mine
    for copy in halos + lat_copies + lon_copies:
        copy.wait_send()


def put_out(*refs):
    sem = refs[10]
    copies = [pltpu.make_async_copy(refs[i], refs[5 + i], sem.at[i]) for i in range(5)]
    for copy in copies:
        copy.start()
    for copy in copies:
        copy.wait()


def local(n_lat, n_lon, *args):
    args = list(args)
    args[:3] = [jnp.transpose(a, (1, 0, 2)) for a in args[:3]]
    args[11] = args[11].reshape(1, -1)
    rows, cols = args[3].shape
    bands = BANDS_DEV * n_lat
    width = -(-bands // cols) * cols
    tall = rows + 2 * EDGE
    f32 = jnp.float32
    vmem = pl.BlockSpec(memory_space=pltpu.VMEM)
    shapes = [args[i].shape for i in (0, 1, 5, 6)] + [(1, BANDS_DEV)]
    dma = pltpu.SemaphoreType.DMA
    results = pl.pallas_call(
        functools.partial(kernel, n_lat, n_lon),
        out_shape=[pltpu.VMEM(shape, f32) for shape in shapes],
        in_specs=[pl.BlockSpec(memory_space=pl.ANY)] * 12,
        out_specs=[vmem] * 5,
        scratch_shapes=[pltpu.VMEM(a.shape, a.dtype) for a in args]
        + [
            pltpu.VMEM((FIELDS, rows, cols), f32),
            pltpu.VMEM((rows, cols), f32),
            pltpu.VMEM((FIELDS, EDGE, cols), f32),
            pltpu.VMEM((FIELDS, EDGE, cols), f32),
            pltpu.VMEM((tall, cols), f32),
            pltpu.VMEM((tall, cols), f32),
            pltpu.VMEM((n_lat, EDGE, width), f32),
            pltpu.VMEM((n_lon, EDGE, width), f32),
            dma((12,)),
            dma((8,)),
            dma((8,)),
            dma((n_lat - 1,)),
            dma((n_lat - 1,)),
            dma((n_lon - 1,)),
            dma((n_lon - 1,)),
        ],
        compiler_params=pltpu.CompilerParams(collective_id=0, has_side_effects=True),
        name="ice_step",
    )(*args)
    temp, thick, vel, stress, zonal = pl.pallas_call(
        put_out,
        out_shape=[jax.ShapeDtypeStruct(shape, f32) for shape in shapes],
        in_specs=[vmem] * 5,
        out_specs=[pl.BlockSpec(memory_space=pl.ANY)] * 5,
        scratch_shapes=[dma((5,))],
        name="put_out",
    )(*[pltpu.with_memory_space_constraint(r, pltpu.VMEM) for r in results])
    temp, thick = [jnp.transpose(a, (1, 0, 2)) for a in (temp, thick)]
    return (temp, thick, vel, stress, zonal.reshape(BANDS_DEV))


def solution(mesh):
    shape = dict(mesh.shape)
    return jax.shard_map(
        functools.partial(local, shape["lat"], shape["lon"]),
        mesh=mesh,
        in_specs=(
            P("lat", None, "lon"),
            P("lat", None, "lon"),
            P("lat", None, "lon"),
            P("lat", "lon"),
            P("lat", "lon"),
            P(None, "lat", "lon"),
            P(None, "lat", "lon"),
            P(None, "lat", "lon"),
            P(None, "lat", "lon"),
            P("lat", "lon"),
            P("lon", "lat"),
            P("lat"),
        ),
        out_specs=(
            P("lat", None, "lon"),
            P("lat", None, "lon"),
            P(None, "lat", "lon"),
            P(None, "lat", "lon"),
            P("lat"),
        ),
        check_vma=False,
    )
```
